32 devices in a mesh: dp: 2 (over x), tp: 4 (over z), pp: 4 (over y, core).
Axes of the slice: x: 2, y: 2, z: 4, core: 2. Of those that a mesh axis runs over, the one named last changes fastest.
Arguments:
- stage_buf: bfloat16 [4, 16, 512, 2560], P('pp', 'dp', 'tp'), parts along dimension 1
- new_mb: bfloat16 [16, 512, 2560], P('dp', 'tp'), parts along dimension 0
- positions: int32 [512], replicated
- ln_attn: float32 [4, 2, 2560], P('pp')
- ln_mlp: float32 [4, 2, 2560], P('pp')
- w_qkv: bfloat16 [4, 32, 3, 80, 2560], P('pp', 'tp')
- w_out: bfloat16 [4, 2560, 2560], P('pp', 'tp')
- w_up: bfloat16 [4, 2560, 10240], P('pp', None, 'tp')
- w_down: bfloat16 [4, 10240, 2560], P('pp', 'tp')
Outputs:
- output 1: bfloat16 [16, 512, 2560], P('dp', 'tp', 'pp'), parts along dimension 0
- output 2: bfloat16 [16, 512, 2560], P('dp', 'tp', 'pp'), parts along dimension 0
- output 3: bfloat16 [4, 16, 512, 2560], P('pp', 'dp', 'tp'), parts along dimension 1
There are 2 independent parts. The reference program is written for one: setup_inputs(seed, part) draws one part's arguments, and reference() takes and returns one part's arrays. A program takes and returns all parts, laid end to end along the dimension named above; an argument that names none is the same for every part.
All inputs are finite; a program needn't handle non-finite values.
Results may differ from the reference program's by a relative error of at most 0.0179774.
Values are sent between devices in bfloat16 or wider.
A program may use at most 1 GiB of HBM per device.

```python
import jax
import jax.numpy as jnp
from jax import lax

STAGES = 4
MICRO_BATCH = 8
SEQ_LEN = 512
D_MODEL = 2560
N_HEADS = 32
KV_GROUPS = 32
HEAD_DIM = 80
FF_DIM = 10240
LN_EPS = 1e-5
ROPE_BASE = 10000.0


def setup_inputs(seed: int = 0, part: int = 0) -> dict:
    base_key = jax.random.key(seed)
    key_list = jax.random.split(base_key, 8)
    act_keys = jax.random.split(jax.random.fold_in(key_list[7], part), 2)
    groups = N_HEADS // KV_GROUPS
    in_scale = D_MODEL ** -0.5
    stage_buf = jax.random.normal(act_keys[0], (STAGES, MICRO_BATCH, SEQ_LEN, D_MODEL), jnp.float32).astype(jnp.bfloat16)
    new_mb = jax.random.normal(act_keys[1], (MICRO_BATCH, SEQ_LEN, D_MODEL), jnp.float32).astype(jnp.bfloat16)
    pos_steps = jax.random.randint(key_list[0], (SEQ_LEN,), 1, 4)
    offset = jax.random.randint(key_list[1], (), 0, SEQ_LEN)
    positions = (offset + jnp.cumsum(pos_steps) - 1).astype(jnp.int32)
    ln_noise = 0.2 * jax.random.normal(key_list[2], (2, STAGES, 2, D_MODEL), jnp.float32)
    ln_base = jnp.array([1.0, 0.0], jnp.float32)[None, :, None]
    w_qkv = (1.5 * in_scale * jax.random.normal(key_list[3], (STAGES, KV_GROUPS, groups + 2, HEAD_DIM, D_MODEL), jnp.float32)).astype(jnp.bfloat16)
    w_out = (in_scale * jax.random.normal(key_list[4], (STAGES, D_MODEL, D_MODEL), jnp.float32)).astype(jnp.bfloat16)
    w_up = (in_scale * jax.random.normal(key_list[5], (STAGES, D_MODEL, FF_DIM), jnp.float32)).astype(jnp.bfloat16)
    w_down = (FF_DIM ** -0.5 * jax.random.normal(key_list[6], (STAGES, FF_DIM, D_MODEL), jnp.float32)).astype(jnp.bfloat16)
    return {"stage_buf": stage_buf, "new_mb": new_mb, "positions": positions, "ln_attn": ln_base + ln_noise[0], "ln_mlp": ln_base + ln_noise[1], "w_qkv": w_qkv, "w_out": w_out, "w_up": w_up, "w_down": w_down}


def rope_tables(positions):
    inv_freq = 1.0 / (ROPE_BASE ** (jnp.arange(0, HEAD_DIM, 2).astype(jnp.float32) / HEAD_DIM))
    angles = positions.astype(jnp.float32)[:, None] * inv_freq[None, :]
    return jnp.cos(angles), jnp.sin(angles)


def layer_norm(x_in, ln_params):
    x_wide = x_in.astype(jnp.float32)
    centered = x_wide - jnp.mean(x_wide, axis=-1, keepdims=True)
    variance = jnp.mean(jnp.square(centered), axis=-1, keepdims=True)
    return (centered * lax.rsqrt(variance + LN_EPS) * ln_params[0] + ln_params[1]).astype(jnp.bfloat16)


def rotate_half(x_in, cos_tab, sin_tab):
    half_dim = x_in.shape[-1] // 2
    x_wide = x_in.astype(jnp.float32)
    first_half = x_wide[..., :half_dim]
    second_half = x_wide[..., half_dim:]
    return jnp.concatenate([first_half * cos_tab - second_half * sin_tab, second_half * cos_tab + first_half * sin_tab], axis=-1).astype(jnp.bfloat16)


def apply_layer(x_in, ln_attn, ln_mlp, w_qkv, w_out, w_up, w_down, cos_tab, sin_tab):
    groups = N_HEADS // KV_GROUPS
    a_norm = layer_norm(x_in, ln_attn).reshape(MICRO_BATCH * SEQ_LEN, D_MODEL)
    m_norm = layer_norm(x_in, ln_mlp).reshape(MICRO_BATCH * SEQ_LEN, D_MODEL)
    qkv_proj = jnp.dot(a_norm, w_qkv.reshape(-1, D_MODEL).T, preferred_element_type=jnp.float32).astype(jnp.bfloat16)
    qkv_proj = qkv_proj.reshape(MICRO_BATCH, SEQ_LEN, KV_GROUPS, groups + 2, HEAD_DIM)
    queries = rotate_half(qkv_proj[:, :, :, :groups], cos_tab[:, None, None], sin_tab[:, None, None])
    key_rot = rotate_half(qkv_proj[:, :, :, groups], cos_tab[:, None], sin_tab[:, None])
    values = qkv_proj[:, :, :, groups + 1]
    scores = jnp.einsum("bskgh,btkh->bkgst", queries.astype(jnp.float32), key_rot.astype(jnp.float32)) * HEAD_DIM ** -0.5
    causal = jnp.arange(SEQ_LEN)[:, None] >= jnp.arange(SEQ_LEN)[None, :]
    attn_probs = jax.nn.softmax(jnp.where(causal, scores, -1e30), axis=-1).astype(jnp.bfloat16)
    attn_heads = jnp.einsum("bkgst,btkh->bskgh", attn_probs.astype(jnp.float32), values.astype(jnp.float32)).astype(jnp.bfloat16)
    attn_part = jnp.dot(attn_heads.reshape(MICRO_BATCH * SEQ_LEN, D_MODEL), w_out, preferred_element_type=jnp.float32)
    hidden = jax.nn.gelu(jnp.dot(m_norm, w_up, preferred_element_type=jnp.float32), approximate=False).astype(jnp.bfloat16)
    mlp_part = jnp.dot(hidden, w_down, preferred_element_type=jnp.float32)
    summed = x_in.astype(jnp.float32) + (attn_part + mlp_part).reshape(MICRO_BATCH, SEQ_LEN, D_MODEL)
    return summed.astype(jnp.bfloat16)


def reference(stage_buf, new_mb, positions, ln_attn, ln_mlp, w_qkv, w_out, w_up, w_down):
    cos_tab, sin_tab = rope_tables(positions)

    def layer_step(stage_item):
        return apply_layer(stage_item[0], stage_item[1], stage_item[2], stage_item[3], stage_item[4], stage_item[5], stage_item[6], cos_tab, sin_tab)

    def run_tick(stage_bufs):
        return lax.map(layer_step, (stage_bufs, ln_attn, ln_mlp, w_qkv, w_out, w_up, w_down))

    out_one = run_tick(stage_buf)
    buf_one = jnp.concatenate([new_mb[None], out_one[:-1]], axis=0)
    out_two = run_tick(buf_one)
    final_buf = jnp.concatenate([jnp.zeros_like(new_mb)[None], out_two[:-1]], axis=0)
    return (out_one[-1], out_two[-1], final_buf)
```

```python
import functools

import jax
import jax.numpy as jnp
from jax import lax
from jax.experimental import pallas as pl
from jax.experimental.pallas import tpu as pltpu
from jax.sharding import PartitionSpec as P


LN_EPS = 1e-5
ROPE_BASE = 10000.0
CHUNKS = 4


def rope_tables(positions, head_dim):
    inv_freq = 1.0 / (ROPE_BASE ** (jnp.arange(0, head_dim, 2).astype(jnp.float32) / head_dim))
    angles = positions.astype(jnp.float32)[:, None] * inv_freq[None, :]
    return jnp.cos(angles), jnp.sin(angles)


def rotate_half(x_in, cos_tab, sin_tab):
    half_dim = x_in.shape[-1] // 2
    x_wide = x_in.astype(jnp.float32)
    first_half = x_wide[..., :half_dim]
    second_half = x_wide[..., half_dim:]
    return jnp.concatenate([first_half * cos_tab - second_half * sin_tab, second_half * cos_tab + first_half * sin_tab], axis=-1).astype(jnp.bfloat16)


def norm_kernel(n, rank_ref, *refs):
    own_ref, from_left, from_right = refs[0], refs[1:n], refs[n : 2 * n - 1]
    ln_ref, a_ref, m_ref = refs[2 * n - 1 :]
    k = pl.program_id(1)
    rank = rank_ref[0]

    def write(x_ref):
        x_wide = x_ref[0].astype(jnp.float32)
        centered = x_wide - jnp.mean(x_wide, axis=-1, keepdims=True)
        variance = jnp.mean(jnp.square(centered), axis=-1, keepdims=True)
        normed = centered * lax.rsqrt(variance + LN_EPS)
        a_ref[0] = (normed * ln_ref[0:1, :] + ln_ref[1:2, :]).astype(jnp.bfloat16)
        m_ref[0] = (normed * ln_ref[2:3, :] + ln_ref[3:4, :]).astype(jnp.bfloat16)

    pl.when(k == 0)(lambda: write(own_ref))
    for step in range(1, n):
        pl.when(jnp.logical_and(k == step, rank >= step))(lambda: write(from_left[step - 1]))
        pl.when(jnp.logical_and(k == step, rank < step))(lambda: write(from_right[n - step - 1]))


def both_norms(rank, own, from_left, from_right, ln_rows):
    n = len(from_left) + 1
    seqs, rows, width = own.shape
    piece = pl.BlockSpec((1, rows, width), lambda b, k, rank: (b, 0, 0))
    out = pl.BlockSpec((1, rows, width), lambda b, k, rank: (b, k, 0))
    shape = jax.ShapeDtypeStruct((seqs, n * rows, width), jnp.bfloat16)
    return pl.pallas_call(
        functools.partial(norm_kernel, n),
        grid_spec=pltpu.PrefetchScalarGridSpec(
            num_scalar_prefetch=1,
            grid=(seqs, n),
            in_specs=[piece] * (2 * n - 1) + [pl.BlockSpec((4, width), lambda b, k, rank: (0, 0))],
            out_specs=[out, out],
        ),
        out_shape=[shape, shape],
        cost_estimate=pl.CostEstimate(flops=40 * seqs * n * rows * width * 100, bytes_accessed=2 * (4 * n - 1) * seqs * rows * width, transcendentals=0),
        name="both_norms",
    )(rank, own, *from_left, *from_right, ln_rows)


def down_kernel(n, rank_ref, o_ref, g_ref, w_out_ref, w_down_ref, *p_refs):
    seqs, rows = p_refs[0].shape[0], p_refs[0].shape[1]
    part = jnp.dot(g_ref[...], w_down_ref[...], preferred_element_type=jnp.float32)
    part += jnp.dot(o_ref[...], w_out_ref[...], preferred_element_type=jnp.float32)
    part = part.astype(jnp.bfloat16)
    for b in range(seqs):
        for k in range(n):
            start = (b * n + k) * rows
            p_refs[k][b] = part[start : start + rows]

    def first_send(k):
        for b in range(seqs):
            p_refs[n][b] = p_refs[k][b]

    pl.when(rank_ref[0] == 0)(lambda: first_send(1))
    pl.when(rank_ref[0] != 0)(lambda: first_send(n - 1))


def out_and_down(rank, n, seqs, heads_out, hidden, w_out, w_down, block=512):
    tokens, width = hidden.shape[0], w_down.shape[1]
    rows = tokens // (n * seqs)
    return pl.pallas_call(
        functools.partial(down_kernel, n),
        grid_spec=pltpu.PrefetchScalarGridSpec(
            num_scalar_prefetch=1,
            grid=(width // block,),
            in_specs=[
                pl.BlockSpec((tokens, heads_out.shape[1]), lambda j, rank: (0, 0)),
                pl.BlockSpec((tokens, hidden.shape[1]), lambda j, rank: (0, 0)),
                pl.BlockSpec((w_out.shape[0], block), lambda j, rank: (0, j)),
                pl.BlockSpec((w_down.shape[0], block), lambda j, rank: (0, j)),
            ],
            out_specs=[pl.BlockSpec((seqs, rows, block), lambda j, rank: (0, 0, j))] * (n + 1),
        ),
        out_shape=[jax.ShapeDtypeStruct((seqs, rows, width), jnp.bfloat16)] * (n + 1),
        compiler_params=pltpu.CompilerParams(vmem_limit_bytes=56 * 1024 * 1024),
        cost_estimate=pl.CostEstimate(flops=2 * tokens * width * (w_out.shape[0] + w_down.shape[0]), bytes_accessed=2 * (w_out.size + w_down.size + hidden.size + heads_out.size + tokens * width), transcendentals=0),
        name="out_and_down",
    )(rank, heads_out, hidden, w_out, w_down)


def line_gather(x_loc, n):
    from_left, from_right = [x_loc], [x_loc]
    for step in range(1, n):
        from_left.append(lax.ppermute(from_left[-1], "tp", [(z, z + 1) for z in range(step - 1, n - 1)]))
        from_right.append(lax.ppermute(from_right[-1], "tp", [(z, z - 1) for z in range(1, n - step + 1)]))
    return from_left[1:], from_right[1:]


def line_scatter(parts, first_send):
    inward = lax.ppermute(first_send, "tp", [(0, 1), (3, 2)])
    middle = parts[2] + inward
    rightward = lax.ppermute(middle, "tp", [(0, 1), (1, 2)])
    leftward = lax.ppermute(middle, "tp", [(3, 2), (2, 1)])
    send_right, send_left = parts[3] + rightward, parts[1] + leftward
    rightward = lax.ppermute(send_right, "tp", [(0, 1), (1, 2), (2, 3)])
    leftward = lax.ppermute(send_left, "tp", [(3, 2), (2, 1), (1, 0)])
    return parts[0].astype(jnp.float32) + rightward.astype(jnp.float32) + leftward.astype(jnp.float32)


def attention_heads(a_norm, w_qkv, cos_tab, sin_tab, causal):
    groups = w_qkv.shape[1] - 2
    head_dim = w_qkv.shape[2]
    qkv_proj = jnp.einsum("nsd,kjhd->nskjh", a_norm, w_qkv, preferred_element_type=jnp.float32).astype(jnp.bfloat16)
    queries = rotate_half(qkv_proj[:, :, :, :groups], cos_tab[:, None, None], sin_tab[:, None, None])
    key_rot = rotate_half(qkv_proj[:, :, :, groups], cos_tab[:, None], sin_tab[:, None])
    values = qkv_proj[:, :, :, groups + 1]
    scores = jnp.einsum("nskgh,ntkh->nkgst", queries, key_rot, preferred_element_type=jnp.float32) * head_dim ** -0.5
    attn_probs = jax.nn.softmax(jnp.where(causal, scores, -1e30), axis=-1).astype(jnp.bfloat16)
    return jnp.einsum("nkgst,ntkh->nskgh", attn_probs, values, preferred_element_type=jnp.float32).astype(jnp.bfloat16)


def solution(mesh):
    stages = mesh.shape["pp"]
    n = mesh.shape["tp"]
    shift_pairs = [(src_stage, src_stage + 1) for src_stage in range(stages - 1)]
    act_spec = P("dp", "tp", None)
    buf_spec = P("pp", "dp", "tp", None)
    emit_spec = P("dp", "tp", "pp")
    stack_spec = P("pp", None, None)

    def stage_body(stage_buf, new_mb, positions, ln_attn, ln_mlp, w_qkv, w_out, w_up, w_down):
        stage_idx = lax.axis_index("pp")
        rank = lax.axis_index("tp")
        seqs = stage_buf.shape[1] // CHUNKS
        rows, width = stage_buf.shape[2], stage_buf.shape[3]
        order = (rank + n - jnp.arange(n)) % n
        token_idx = (order[:, None] * rows + jnp.arange(rows)[None, :]).reshape(-1)
        cos_tab, sin_tab = rope_tables(positions[token_idx], w_qkv.shape[3])
        causal = token_idx[:, None] >= token_idx[None, :]
        ln_rows = jnp.concatenate([ln_attn[0], ln_mlp[0]], axis=0)
        rank_arr = rank.astype(jnp.int32)[None]

        def layer_here(x_loc):
            from_left, from_right = line_gather(x_loc, n)
            a_norm, m_norm = both_norms(rank_arr, x_loc, from_left, from_right, ln_rows)
            a_norm, cos_here, sin_here, causal_here = lax.optimization_barrier((a_norm, cos_tab, sin_tab, causal))
            heads_out = attention_heads(a_norm, w_qkv[0], cos_here, sin_here, causal_here)
            hidden = jnp.dot(m_norm.reshape(-1, width), w_up[0], preferred_element_type=jnp.float32)
            hidden = jax.nn.gelu(hidden, approximate=False).astype(jnp.bfloat16)
            *parts, first_send = out_and_down(rank_arr, n, seqs, heads_out.reshape(seqs * n * rows, -1), hidden, w_out[0], w_down[0])
            x_late, parts = lax.optimization_barrier((x_loc, parts))
            reduced = line_scatter(parts, first_send)
            return (x_late.astype(jnp.float32) + reduced).astype(jnp.bfloat16)

        def emit_last(y_list):
            block = width // stages

            def columns(dst):
                return jnp.concatenate([y[..., dst * block : (dst + 1) * block] for y in y_list])

            mine = jnp.where(stage_idx == stages - 1, columns(stages - 1), jnp.zeros((), y_list[0].dtype))
            for dst in range(stages - 1):
                mine = mine + lax.ppermute(columns(dst), "pp", [(stages - 1, dst)])
            return mine

        def shift(y_loc):
            return lax.ppermute(y_loc, "pp", shift_pairs)

        first, second, bufs, final_buf = [], [], [], []
        for c in range(CHUNKS):
            first.append(layer_here(stage_buf[0, c * seqs : (c + 1) * seqs]))
            shifted, fresh = lax.optimization_barrier((shift(first[c]), new_mb[c * seqs : (c + 1) * seqs]))
            bufs.append(jnp.where(stage_idx == 0, fresh, shifted))
        emit_one = emit_last(first)
        for c in range(CHUNKS):
            second.append(layer_here(bufs[c]))
            final_buf.append(shift(second[c]))
        emit_two = jnp.concatenate([emit_last(second[:-1]), emit_last(second[-1:])])
        return emit_one, emit_two, jnp.concatenate(final_buf)[None]

    return jax.shard_map(stage_body, mesh=mesh, in_specs=(buf_spec, act_spec, P(None), stack_spec, stack_spec, P("pp", "tp", None, None, None), P("pp", "tp", None), P("pp", None, "tp"), P("pp", "tp", None)), out_specs=(emit_spec, emit_spec, buf_spec), check_vma=False)
```

```python
import functools

import jax
import jax.numpy as jnp
from jax import lax
from jax.experimental import pallas as pl
from jax.experimental.pallas import tpu as pltpu
from jax.sharding import PartitionSpec as P


LN_EPS = 1e-5
ROPE_BASE = 10000.0
CHUNKS = 4


def rope_tables(positions, head_dim):
    inv_freq = 1.0 / (ROPE_BASE ** (jnp.arange(0, head_dim, 2).astype(jnp.float32) / head_dim))
    angles = positions.astype(jnp.float32)[:, None] * inv_freq[None, :]
    return jnp.cos(angles), jnp.sin(angles)


def rotate_half(x_in, cos_tab, sin_tab):
    half_dim = x_in.shape[-1] // 2
    x_wide = x_in.astype(jnp.float32)
    first_half = x_wide[..., :half_dim]
    second_half = x_wide[..., half_dim:]
    return jnp.concatenate([first_half * cos_tab - second_half * sin_tab, second_half * cos_tab + first_half * sin_tab], axis=-1).astype(jnp.bfloat16)


def norm_kernel(n, rank_ref, *refs):
    own_ref, from_left, from_right = refs[0], refs[1:n], refs[n : 2 * n - 1]
    ln_ref, a_ref, m_ref = refs[2 * n - 1 :]
    k = pl.program_id(1)
    rank = rank_ref[0]

    def write(x_ref):
        x_wide = x_ref[0].astype(jnp.float32)
        centered = x_wide - jnp.mean(x_wide, axis=-1, keepdims=True)
        variance = jnp.mean(jnp.square(centered), axis=-1, keepdims=True)
        normed = centered * lax.rsqrt(variance + LN_EPS)
        a_ref[0] = (normed * ln_ref[0:1, :] + ln_ref[1:2, :]).astype(jnp.bfloat16)
        m_ref[0] = (normed * ln_ref[2:3, :] + ln_ref[3:4, :]).astype(jnp.bfloat16)

    pl.when(k == 0)(lambda: write(own_ref))
    for step in range(1, n):
        pl.when(jnp.logical_and(k == step, rank >= step))(lambda: write(from_left[step - 1]))
        pl.when(jnp.logical_and(k == step, rank < step))(lambda: write(from_right[n - step - 1]))


def both_norms(rank, own, from_left, from_right, ln_rows):
    n = len(from_left) + 1
    seqs, rows, width = own.shape
    piece = pl.BlockSpec((1, rows, width), lambda b, k, rank: (b, 0, 0))
    out = pl.BlockSpec((1, rows, width), lambda b, k, rank: (b, k, 0))
    shape = jax.ShapeDtypeStruct((seqs, n * rows, width), jnp.bfloat16)
    return pl.pallas_call(
        functools.partial(norm_kernel, n),
        grid_spec=pltpu.PrefetchScalarGridSpec(
            num_scalar_prefetch=1,
            grid=(seqs, n),
            in_specs=[piece] * (2 * n - 1) + [pl.BlockSpec((4, width), lambda b, k, rank: (0, 0))],
            out_specs=[out, out],
        ),
        out_shape=[shape, shape],
        cost_estimate=pl.CostEstimate(flops=40 * seqs * n * rows * width * 100, bytes_accessed=2 * (4 * n - 1) * seqs * rows * width, transcendentals=0),
        name="both_norms",
    )(rank, own, *from_left, *from_right, ln_rows)


def up_kernel(pieces, m_ref, w_up_ref, g_ref):
    rows = m_ref.shape[0] // pieces
    for piece in range(pieces):
        at = slice(piece * rows, (piece + 1) * rows)
        wide = jnp.dot(m_ref[at, :], w_up_ref[...], preferred_element_type=jnp.float32)
        g_ref[at, :] = (0.5 * wide * (1.0 + lax.erf(wide * 0.5**0.5))).astype(jnp.bfloat16)


def up_and_gelu(m_norm, w_up, block=512, pieces=2):
    tokens, width = m_norm.shape
    return pl.pallas_call(
        functools.partial(up_kernel, pieces),
        grid=(w_up.shape[1] // block,),
        in_specs=[pl.BlockSpec((tokens, width), lambda j: (0, 0)), pl.BlockSpec((width, block), lambda j: (0, j))],
        out_specs=pl.BlockSpec((tokens, block), lambda j: (0, j)),
        out_shape=jax.ShapeDtypeStruct((tokens, w_up.shape[1]), jnp.bfloat16),
        compiler_params=pltpu.CompilerParams(vmem_limit_bytes=48 * 1024 * 1024),
        cost_estimate=pl.CostEstimate(flops=2 * tokens * w_up.size, bytes_accessed=2 * (w_up.size + m_norm.size + tokens * w_up.shape[1]), transcendentals=tokens * w_up.shape[1]),
        name="up_and_gelu",
    )(m_norm, w_up)


def down_kernel(n, rank_ref, o_ref, g_ref, w_out_ref, w_down_ref, *p_refs):
    seqs, rows = p_refs[0].shape[0], p_refs[0].shape[1]
    part = jnp.dot(g_ref[...], w_down_ref[...], preferred_element_type=jnp.float32)
    part += jnp.dot(o_ref[...], w_out_ref[...], preferred_element_type=jnp.float32)
    part = part.astype(jnp.bfloat16)
    for b in range(seqs):
        for k in range(n):
            start = (b * n + k) * rows
            p_refs[k][b] = part[start : start + rows]

    def first_send(k):
        for b in range(seqs):
            p_refs[n][b] = p_refs[k][b]

    pl.when(rank_ref[0] == 0)(lambda: first_send(1))
    pl.when(rank_ref[0] != 0)(lambda: first_send(n - 1))


def out_and_down(rank, n, seqs, heads_out, hidden, w_out, w_down, block=512):
    tokens, width = hidden.shape[0], w_down.shape[1]
    rows = tokens // (n * seqs)
    return pl.pallas_call(
        functools.partial(down_kernel, n),
        grid_spec=pltpu.PrefetchScalarGridSpec(
            num_scalar_prefetch=1,
            grid=(width // block,),
            in_specs=[
                pl.BlockSpec((tokens, heads_out.shape[1]), lambda j, rank: (0, 0)),
                pl.BlockSpec((tokens, hidden.shape[1]), lambda j, rank: (0, 0)),
                pl.BlockSpec((w_out.shape[0], block), lambda j, rank: (0, j)),
                pl.BlockSpec((w_down.shape[0], block), lambda j, rank: (0, j)),
            ],
            out_specs=[pl.BlockSpec((seqs, rows, block), lambda j, rank: (0, 0, j))] * (n + 1),
        ),
        out_shape=[jax.ShapeDtypeStruct((seqs, rows, width), jnp.bfloat16)] * (n + 1),
        compiler_params=pltpu.CompilerParams(vmem_limit_bytes=56 * 1024 * 1024),
        cost_estimate=pl.CostEstimate(flops=2 * tokens * width * (w_out.shape[0] + w_down.shape[0]), bytes_accessed=2 * (w_out.size + w_down.size + hidden.size + heads_out.size + tokens * width), transcendentals=0),
        name="out_and_down",
    )(rank, heads_out, hidden, w_out, w_down)


def line_gather(x_loc, n):
    from_left, from_right = [x_loc], [x_loc]
    for step in range(1, n):
        from_left.append(lax.ppermute(from_left[-1], "tp", [(z, z + 1) for z in range(step - 1, n - 1)]))
        from_right.append(lax.ppermute(from_right[-1], "tp", [(z, z - 1) for z in range(1, n - step + 1)]))
    return from_left[1:], from_right[1:]


def line_scatter(parts, first_send):
    inward = lax.ppermute(first_send, "tp", [(0, 1), (3, 2)])
    middle = parts[2] + inward
    rightward = lax.ppermute(middle, "tp", [(0, 1), (1, 2)])
    leftward = lax.ppermute(middle, "tp", [(3, 2), (2, 1)])
    send_right, send_left = parts[3] + rightward, parts[1] + leftward
    rightward = lax.ppermute(send_right, "tp", [(0, 1), (1, 2), (2, 3)])
    leftward = lax.ppermute(send_left, "tp", [(3, 2), (2, 1), (1, 0)])
    return parts[0].astype(jnp.float32) + rightward.astype(jnp.float32) + leftward.astype(jnp.float32)


def attention_heads(a_norm, w_qkv, cos_tab, sin_tab, causal):
    groups = w_qkv.shape[1] - 2
    head_dim = w_qkv.shape[2]
    qkv_proj = jnp.einsum("nsd,kjhd->nskjh", a_norm, w_qkv, preferred_element_type=jnp.float32).astype(jnp.bfloat16)
    queries = rotate_half(qkv_proj[:, :, :, :groups], cos_tab[:, None, None], sin_tab[:, None, None])
    key_rot = rotate_half(qkv_proj[:, :, :, groups], cos_tab[:, None], sin_tab[:, None])
    values = qkv_proj[:, :, :, groups + 1]
    scores = jnp.einsum("nskgh,ntkh->nkgst", queries, key_rot, preferred_element_type=jnp.float32) * head_dim ** -0.5
    attn_probs = jax.nn.softmax(jnp.where(causal, scores, -1e30), axis=-1).astype(jnp.bfloat16)
    return jnp.einsum("nkgst,ntkh->nskgh", attn_probs, values, preferred_element_type=jnp.float32).astype(jnp.bfloat16)


def solution(mesh):
    stages = mesh.shape["pp"]
    n = mesh.shape["tp"]
    shift_pairs = [(src_stage, src_stage + 1) for src_stage in range(stages - 1)]
    act_spec = P("dp", "tp", None)
    buf_spec = P("pp", "dp", "tp", None)
    emit_spec = P("dp", "tp", "pp")
    stack_spec = P("pp", None, None)

    def stage_body(stage_buf, new_mb, positions, ln_attn, ln_mlp, w_qkv, w_out, w_up, w_down):
        stage_idx = lax.axis_index("pp")
        rank = lax.axis_index("tp")
        seqs = stage_buf.shape[1] // CHUNKS
        rows, width = stage_buf.shape[2], stage_buf.shape[3]
        order = (rank + n - jnp.arange(n)) % n
        token_idx = (order[:, None] * rows + jnp.arange(rows)[None, :]).reshape(-1)
        cos_tab, sin_tab = rope_tables(positions[token_idx], w_qkv.shape[3])
        causal = token_idx[:, None] >= token_idx[None, :]
        ln_rows = jnp.concatenate([ln_attn[0], ln_mlp[0]], axis=0)
        rank_arr = rank.astype(jnp.int32)[None]

        def layer_here(x_loc):
            from_left, from_right = line_gather(x_loc, n)
            a_norm, m_norm = both_norms(rank_arr, x_loc, from_left, from_right, ln_rows)
            a_norm, cos_here, sin_here, causal_here = lax.optimization_barrier((a_norm, cos_tab, sin_tab, causal))
            heads_out = attention_heads(a_norm, w_qkv[0], cos_here, sin_here, causal_here)
            hidden = up_and_gelu(m_norm.reshape(-1, width), w_up[0])
            *parts, first_send = out_and_down(rank_arr, n, seqs, heads_out.reshape(seqs * n * rows, -1), hidden, w_out[0], w_down[0])
            x_late, parts = lax.optimization_barrier((x_loc, parts))
            reduced = line_scatter(parts, first_send)
            return (x_late.astype(jnp.float32) + reduced).astype(jnp.bfloat16)

        def emit_last(y_list):
            block = width // stages

            def columns(dst):
                return jnp.concatenate([y[..., dst * block : (dst + 1) * block] for y in y_list])

            mine = jnp.where(stage_idx == stages - 1, columns(stages - 1), jnp.zeros((), y_list[0].dtype))
            for dst in range(stages - 1):
                mine = mine + lax.ppermute(columns(dst), "pp", [(stages - 1, dst)])
            return mine

        def shift(y_loc):
            return lax.ppermute(y_loc, "pp", shift_pairs)

        first, second, bufs, final_buf = [], [], [], []
        for c in range(CHUNKS):
            first.append(layer_here(stage_buf[0, c * seqs : (c + 1) * seqs]))
            shifted, fresh = lax.optimization_barrier((shift(first[c]), new_mb[c * seqs : (c + 1) * seqs]))
            bufs.append(jnp.where(stage_idx == 0, fresh, shifted))
        emit_one = emit_last(first)
        for c in range(CHUNKS):
            second.append(layer_here(bufs[c]))
            final_buf.append(shift(second[c]))
        emit_two = jnp.concatenate([emit_last(second[:-1]), emit_last(second[-1:])])
        return emit_one, emit_two, jnp.concatenate(final_buf)[None]

    return jax.shard_map(stage_body, mesh=mesh, in_specs=(buf_spec, act_spec, P(None), stack_spec, stack_spec, P("pp", "tp", None, None, None), P("pp", "tp", None), P("pp", None, "tp"), P("pp", "tp", None)), out_specs=(emit_spec, emit_spec, buf_spec), check_vma=False)
```
